32 devices in a mesh: row: 16 (over z, x, core), ga: 2 (over y).
Axes of the slice: x: 2, y: 2, z: 4, core: 2. Of those that a mesh axis runs over, the one named last changes fastest.
Arguments:
- pair_dens: bfloat16 [16, 256, 4096], P('row', None, 'ga'), may hold values from -0.41992188 to 0.41992188
- cond_dens: bfloat16 [16, 1024, 4096], P('row', None, 'ga'), may hold values from -0.41992188 to 0.41992188
- val_dens: bfloat16 [16, 64, 4096], P(None, None, 'row'), may hold values from -0.41992188 to 0.41992188
- screened: bfloat16 [8, 4096, 4096], P(None, 'ga', 'row'), may hold values from -1 to 6, as said below
- coulomb: bfloat16 [4096], P('ga'), may hold values from 0.29882812 to 10
- pair_list: int32 [16, 256], replicated, may hold values from 0 to 255, each once within a row
- counts: int32 [16], replicated, may hold values from 10 to 256
- q_index: int32 [16], replicated, may hold values from 0 to 7
- column_k: int32 [1], replicated, may hold values from 0 to 15
Outputs:
- kernel: bfloat16 [4096, 256], P('row', 'ga')
The draws below stay inside these ranges and needn't reach their ends.
Inputs may be any that keep to these rules, and one draw needn't show every extreme that they name: `screened`: each diagonal entry exceeds the sum of the magnitudes of the others in its row divided by the square root of 4096 times four.
All inputs are finite; a program needn't handle non-finite values.
Results may differ from the reference program's by a relative error of at most 0.0042.
Values may be sent and summed in bfloat16 or wider, within the bound.
A program may use at most 128 MiB of HBM per device.

```python
import math
import jax
import jax.numpy as jnp
from jax import lax

NV = 8
NC = 32
G = 4096
NQ = 8
PMAX = 256
VV = 64
NK = 16


def draw_screened(key, part):
    first = jax.random.fold_in(key, 11)
    second = jax.random.fold_in(key, 12)
    noise = jnp.clip(jax.random.normal(first, (NQ, G, G)), -4.0, 4.0)
    diag = jnp.exp(jax.random.uniform(second, (NQ, G), minval=0.0, maxval=math.log(5.0)))
    same = jnp.arange(G)[:, None] == jnp.arange(G)[None, :]
    return (noise / math.sqrt(G) + jnp.where(same[None, :, :], diag[:, :, None], 0.0)).astype(jnp.bfloat16)


def place_ends(result, own_key, smallest, top_value):
    dims = result.shape
    index_at = [jax.random.randint(jax.random.fold_in(own_key, axis), (), 0, dims[axis]) for axis in range(len(dims))]
    result = result.at[tuple(index_at)].set(smallest)
    longest = dims.index(max(dims))
    index_at[longest] = (index_at[longest] + 1) % dims[longest]
    return result.at[tuple(index_at)].set(top_value)


def shard_levels(stream_key, shape, shards, low, largest):
    def one(dim, shards_of):
        draws = jax.random.uniform(jax.random.fold_in(jax.random.fold_in(stream_key, 6), dim), (shards_of,), jnp.float32, low / len(shards), largest / len(shards))
        return jnp.repeat(jnp.exp(draws), shape[dim] // shards_of).reshape((-1,) + (1,) * (len(shape) - dim - 1))

    loudness = one(*shards[0])
    for cut in shards[1:]:
        loudness = loudness * one(*cut)
    return loudness


def gaussian(rng, extent, width, limit, pieces=(), kind=jnp.bfloat16):
    result = width * jax.random.normal(rng, extent, jnp.float32)
    if pieces:
        result = result * shard_levels(rng, extent, pieces, -0.22, 0.18)
    return jnp.clip(result, -limit, limit).astype(kind)


def setup_inputs(seed: int = 0) -> dict:
    keys = jax.random.split(jax.random.key(seed), 10)
    pair_dens = gaussian(keys[0], (NK, PMAX, G), 0.07, 0.41992188, ((0, 16), (2, 2)))
    cond_dens = gaussian(keys[1], (NK, NC * NC, G), 0.07, 0.41992188, ((0, 16), (2, 2)))
    val_dens = gaussian(keys[2], (NK, VV, G), 0.07, 0.41992188, ((2, 16),))
    screened = draw_screened(jax.random.fold_in(keys[9], 71), 0)
    coulomb = jnp.clip(jnp.exp(math.log(10.0) - 3.5104718 * jax.random.uniform(keys[4], (G,), jnp.float32) ** shard_levels(keys[4], (G,), ((0, 2),), -0.2, 0.2)), 0.29882812, 10.0).astype(jnp.bfloat16)
    pair_list = jax.vmap(lambda own: jax.random.permutation(own, PMAX))(jax.random.split(keys[5], NK)).reshape((NK, PMAX)).astype(jnp.int32)
    counts = place_ends(jax.random.randint(keys[6], (NK,), max(2, NV * NC // 25), min(401, NV * NC + 1)), jax.random.fold_in(keys[6], 1), max(2, NV * NC // 25), (min(401, NV * NC + 1)) - 1).astype(jnp.int32)
    q_index = place_ends(jax.random.randint(keys[7], (NK,), 0, NQ), jax.random.fold_in(keys[7], 1), 0, NQ - 1).astype(jnp.int32)
    column_k = jax.random.randint(keys[8], (1,), 0, NK).astype(jnp.int32)
    return {"pair_dens": pair_dens, "cond_dens": cond_dens, "val_dens": val_dens, "screened": screened, "coulomb": coulomb, "pair_list": pair_list, "counts": counts, "q_index": q_index, "column_k": column_k}


def reference(pair_dens, cond_dens, val_dens, screened, coulomb, pair_list, counts, q_index, column_k):
    column = column_k[0]
    col_pairs = pair_list[column]
    col = jnp.take(pair_dens[column], col_pairs, axis=0)
    col_count = counts[column]
    slots = jnp.arange(NV * NC, dtype=jnp.int32)
    col_mask = (slots < col_count).astype(jnp.float32)

    def one_point(index):
        pairs = pair_list[index]
        rows = jnp.take(pair_dens[index], pairs, axis=0)
        weighted = (rows.astype(jnp.float32) * coulomb.astype(jnp.float32)[None, :]).astype(jnp.bfloat16)
        exch = jnp.dot(weighted, col.T, preferred_element_type=jnp.float32)
        wmat = screened[q_index[index]]
        screened_val = jnp.dot(val_dens[index], wmat.T, preferred_element_type=jnp.float32).astype(jnp.bfloat16)
        direct_full = jnp.dot(cond_dens[index], screened_val.T, preferred_element_type=jnp.float32)
        arranged = direct_full.reshape(NC, NC, NV, NV).transpose(2, 0, 3, 1).reshape(NV * NC, NV * NC)
        direct = jnp.take(jnp.take(arranged, pairs, axis=0), col_pairs, axis=1)
        row_mask = (slots < counts[index]).astype(jnp.float32)
        block = (2.0 * exch - direct) * row_mask[:, None] * col_mask[None, :]
        return block.astype(jnp.bfloat16)

    blocks = lax.map(one_point, jnp.arange(pair_dens.shape[0], dtype=jnp.int32))
    return blocks.reshape(pair_dens.shape[0] * NV * NC, NV * NC)
```

```python
import functools

import jax
import jax.numpy as jnp
from jax import lax
from jax.experimental import pallas as pl
from jax.experimental.pallas import tpu as pltpu
from jax.sharding import PartitionSpec as P

NV = 8
NC = 32
BF = jnp.bfloat16
F32 = jnp.float32
MESH = pl.DeviceIdType.MESH
NT = (((1,), (1,)), ((), ()))


def split(value):
    high = value.astype(BF)
    return high, (value - high.astype(F32)).astype(BF)


def kernel(
    rows_n, ga_n, cut,
    pd_hbm, cond_hbm, val_hbm, w_hbm, coul_ref, pairs_ref, counts_ref, q_ref, column_ref,
    out_ref,
    pd, cond, val, w, part, send_a, send_b, recv_a, recv_b, send_c, recv_c, col, t_ref, kp, kr,
    load_sem, sa_s, sa_r, sb_s, sb_r, s0_s, s0_r, sc_s, sc_r, g_s, g_r, y_s, y_r,
    recv_0, send_0,
):
    r = lax.axis_index("row")
    ga = lax.axis_index("ga")
    levels = []
    while 1 << len(levels) < rows_n:
        levels.append(1 << len(levels))
    order_a = levels[1:]
    order_b = levels[2:3] + levels[1:2] + levels[3:]
    order_c = levels

    def other(index, j):
        for b in levels:
            if j & b:
                index = index + b - 2 * b * ((r // b) % 2)
        return index

    def k_of(j):
        return other(r, j)

    loads = [
        pltpu.make_async_copy(src, dst, load_sem.at[i])
        for i, (src, dst) in enumerate(
            ((pd_hbm, pd), (val_hbm, val), (w_hbm, w), (cond_hbm, cond))
        )
    ]
    for load in loads:
        load.start()

    barrier = pltpu.get_barrier_semaphore()
    for b in levels:
        pl.semaphore_signal(
            barrier, inc=1, device_id={"row": k_of(b), "ga": ga}, device_id_type=MESH
        )
    for d in range(1, ga_n):
        pl.semaphore_signal(
            barrier, inc=1, device_id={"row": r, "ga": (ga + d) % ga_n}, device_id_type=MESH
        )
    pl.semaphore_wait(barrier, len(levels) + ga_n - 1)

    started = []

    def send(src, dst, ssem, rsem, b):
        copy = pltpu.make_async_remote_copy(
            src_ref=src, dst_ref=dst, send_sem=ssem, recv_sem=rsem,
            device_id={"row": k_of(b), "ga": ga}, device_id_type=MESH,
        )
        copy.start()
        started.append(copy)
        return copy

    copies = {}

    def gather_terms(acc, name, recv, order, j):
        for b in order:
            if j & b:
                return acc, b
            copies[name, j | b].wait_recv()
            acc = acc + recv[j | b].astype(acc.dtype)
        return acc, 0

    column = column_ref[0]
    loads[0].wait()
    is_root = column == r

    def finish_c(j):
        own = pd[k_of(j)]
        own = jnp.where(is_root, own, jnp.zeros_like(own))
        acc, b = gather_terms(own, "c", recv_c, order_c, j)
        if j == 0:
            col[r] = acc
            return
        send_c[j] = acc
        copies["c", j] = send(send_c.at[j], recv_c.at[j], sc_s.at[j], sc_r.at[j], b)

    def finish(name, j):
        if name == "a":
            acc = part[j // 2, :, :cut]
            acc, b = gather_terms(acc, "a", recv_a, order_a, j)
        else:
            acc = part[j // 2, :, cut:]
            acc, b = gather_terms(acc, "b", recv_b, order_b, j)
        if j == 0:
            if name == "a":
                t_ref[:, :cut] = acc.astype(BF)
            else:
                t_ref[:, cut:] = acc.astype(BF)
            return
        if name == "a":
            send_a[j // 2] = acc.astype(BF)
            copies["a", j] = send(send_a.at[j // 2], recv_a.at[j], sa_s.at[j], sa_r.at[j], b)
        else:
            send_b[j // 2] = acc.astype(BF)
            copies["b", j] = send(send_b.at[j // 2], recv_b.at[j], sb_s.at[j], sb_r.at[j], b)

    by_depth = sorted(range(rows_n), key=lambda j: (-bin(j).count("1"), -j))

    def first_bit(order, j):
        for at, b in enumerate(order):
            if j & b:
                return at
        return len(order)

    def level(order, at, even):
        return [j for j in by_depth if (not even or j % 2 == 0) and first_bit(order, j) == at]

    for at in (0, 1):
        for j in level(order_c, at, False):
            finish_c(j)

    loads[1].wait()
    loads[2].wait()

    def partial(j):
        k = k_of(j)
        return lax.dot_general(val[k], w[q_ref[k]], NT, preferred_element_type=F32)

    evens = [j for j in by_depth if j % 2 == 0]

    def odd_step(j):
        send_0[j // 2] = partial(j).astype(BF)
        copies["0", j] = send(
            send_0.at[j // 2], recv_0.at[j // 2], s0_s.at[j // 2], s0_r.at[j // 2], 1
        )

    def even_step(j):
        value = partial(j)
        copies["0", j + 1].wait_recv()
        part[j // 2] = value + recv_0[j // 2].astype(F32)
        for name, order in (("a", order_a), ("b", order_b)):
            if first_bit(order, j) == 0:
                finish(name, j)

    skew = 2
    for step in range(len(evens) + skew):
        if step < len(evens):
            odd_step(evens[step] + 1)
        if step >= skew:
            even_step(evens[step - skew])

    for at in range(1, len(order_a)):
        for j in level(order_c, at + 1, False):
            finish_c(j)
        for name, order in (("a", order_a), ("b", order_b)):
            for j in level(order, at, True):
                finish(name, j)
    finish_c(0)

    held = [0]
    for b in reversed(levels):
        new = []
        for i in held:
            k = k_of(i)
            new.append(
                (i | b, send(col.at[k], col.at[k], g_s.at[i | b], g_r.at[i | b], b))
            )
        for i, copy in new:
            copy.wait_recv()
            held.append(i)

    slots = NV * NC
    h = pd.shape[-1]
    weighted = (pd[...].reshape(slots, h).astype(F32) * coul_ref[...].astype(F32)).astype(BF)
    exch = 2.0 * lax.dot_general(
        weighted, col[...].reshape(slots, h), NT, preferred_element_type=F32
    )
    my_pairs = pairs_ref[pl.ds(r, 1), :]
    col_pairs = pairs_ref[pl.ds(column, 1), :]
    place = lax.broadcasted_iota(jnp.int32, (slots, slots), 0)

    def pick(wanted):
        return jnp.where(place == wanted, 1.0, 0.0).astype(F32)

    rows_of = pick(my_pairs).T.astype(BF)
    rows_of_direct = pick((my_pairs % NC) * NV + my_pairs // NC).T.astype(BF)
    cols_of = pick(col_pairs).astype(BF)

    def chosen(left, value):
        high, low = split(value)
        return jnp.dot(left, high, preferred_element_type=F32) + jnp.dot(
            left, low, preferred_element_type=F32
        )

    total = chosen(rows_of, exch)

    finish("a", 0)
    finish("b", 0)
    loads[3].wait()
    vv = NV * NV
    row_id = lax.broadcasted_iota(jnp.int32, (vv, vv), 0)
    col_id = lax.broadcasted_iota(jnp.int32, (vv, vv), 1)
    swap = jnp.where(col_id == (row_id % NV) * NV + row_id // NV, 1.0, 0.0).astype(BF)
    swapped = jnp.dot(swap, t_ref[...], preferred_element_type=F32).astype(BF)
    direct = lax.dot_general(swapped, cond[...], NT, preferred_element_type=F32)
    arranged = jnp.concatenate(
        [
            jnp.concatenate(
                [
                    direct[vp * NV:(vp + 1) * NV, c * NC:(c + 1) * NC]
                    for vp in range(NV)
                ],
                axis=1,
            )
            for c in range(NC)
        ],
        axis=0,
    )
    total = total - chosen(rows_of_direct, arranged)
    high, low = split(total)
    total = jnp.dot(high, cols_of, preferred_element_type=F32) + jnp.dot(
        low, cols_of, preferred_element_type=F32
    )
    width = slots // ga_n
    for g in range(ga_n):
        kp[g] = total[:, g * width:(g + 1) * width]
    finals = []
    for d in range(1, ga_n):
        to = (ga + d) % ga_n
        copy = pltpu.make_async_remote_copy(
            src_ref=kp.at[to], dst_ref=kr.at[d - 1], send_sem=y_s.at[d - 1], recv_sem=y_r.at[d - 1],
            device_id={"row": r, "ga": to}, device_id_type=MESH,
        )
        copy.start()
        finals.append(copy)
    acc = kp[ga]
    for d, copy in enumerate(finals):
        copy.wait_recv()
        acc = acc + kr[d]
    srow = lax.broadcasted_iota(jnp.int32, (slots, width), 0)
    tcol = lax.broadcasted_iota(jnp.int32, (slots, width), 1) + ga * width
    active = (srow < counts_ref[r]) & (tcol < counts_ref[column])
    out_ref[...] = jnp.where(active, acc, 0.0).astype(BF)
    for copy in started + finals:
        copy.wait_send()


def solution(mesh):
    rows_n, ga_n = mesh.shape["row"], mesh.shape["ga"]

    def per_device(
        pair_dens, cond_dens, val_dens, screened, coulomb, pair_list, counts, q_index, column_k
    ):
        slots, h = pair_dens.shape[1:]
        vv = val_dens.shape[1]
        cut = max(128, (h * 5 // 8) // 128 * 128)
        chunk = slots // rows_n
        half = rows_n // 2
        vmem = pl.BlockSpec(memory_space=pltpu.VMEM)
        smem = pl.BlockSpec(memory_space=pltpu.SMEM)
        hbm = pl.BlockSpec(memory_space=pl.ANY)
        dma = pltpu.SemaphoreType.DMA
        return pl.pallas_call(
            functools.partial(kernel, rows_n, ga_n, cut),
            out_shape=jax.ShapeDtypeStruct((slots, slots // ga_n), BF),
            in_specs=[hbm, hbm, hbm, hbm, vmem, vmem, smem, smem, smem],
            out_specs=vmem,
            scratch_shapes=[
                pltpu.VMEM((rows_n, chunk, h), BF),
                pltpu.VMEM(cond_dens.shape[1:], BF),
                pltpu.VMEM(val_dens.shape, BF),
                pltpu.VMEM(screened.shape, BF),
                pltpu.VMEM((half, vv, h), F32),
                pltpu.VMEM((half, vv, cut), BF),
                pltpu.VMEM((half, vv, h - cut), BF),
                pltpu.VMEM((rows_n, vv, cut), BF),
                pltpu.VMEM((rows_n, vv, h - cut), BF),
                pltpu.VMEM((rows_n, chunk, h), BF),
                pltpu.VMEM((rows_n, chunk, h), BF),
                pltpu.VMEM((rows_n, chunk, h), BF),
                pltpu.VMEM((vv, h), BF),
                pltpu.VMEM((ga_n, slots, slots // ga_n), F32),
                pltpu.VMEM((max(1, ga_n - 1), slots, slots // ga_n), F32),
                dma((4,)),
                dma((rows_n,)), dma((rows_n,)),
                dma((rows_n,)), dma((rows_n,)),
                dma((half,)), dma((half,)),
                dma((rows_n,)), dma((rows_n,)),
                dma((rows_n,)), dma((rows_n,)),
                dma((max(1, ga_n - 1),)), dma((max(1, ga_n - 1),)),
                pltpu.VMEM((half, vv, h), BF),
                pltpu.VMEM((half, vv, h), BF),
            ],
            compiler_params=pltpu.CompilerParams(
                collective_id=0, has_side_effects=True, vmem_limit_bytes=60 * 1024 * 1024
            ),
        )(
            pair_dens.reshape(rows_n, chunk, h),
            cond_dens.reshape(cond_dens.shape[1:]),
            val_dens,
            screened,
            coulomb.reshape(1, h),
            pair_list,
            counts,
            q_index,
            column_k,
        )

    placed = (
        P("row", None, "ga"),
        P("row", None, "ga"),
        P(None, None, "row"),
        P(None, "ga", "row"),
        P("ga"),
        P(),
        P(),
        P(),
        P(),
    )
    return jax.shard_map(
        per_device, mesh=mesh, in_specs=placed, out_specs=P("row", "ga"), check_vma=False
    )
```

```python
import functools

import jax
import jax.numpy as jnp
from jax import lax
from jax.experimental import pallas as pl
from jax.experimental.pallas import tpu as pltpu
from jax.sharding import PartitionSpec as P

NV = 8
NC = 32
BF = jnp.bfloat16
F32 = jnp.float32
MESH = pl.DeviceIdType.MESH
NT = (((1,), (1,)), ((), ()))


def split(value):
    high = value.astype(BF)
    return high, (value - high.astype(F32)).astype(BF)


def kernel(
    rows_n, ga_n, cut,
    pd_hbm, cond_hbm, val_hbm, w_hbm, coul_ref, pairs_ref, counts_ref, q_ref, column_ref,
    out_ref,
    pd, cond, val, w_a, w_b, part_a, part_b, send_a, send_b, recv_a, recv_b,
    send_c, recv_c, col, t_a, t_b, own, kp, kr,
    load_sem, sa_s, sa_r, sb_s, sb_r, sc_s, sc_r, g_s, g_r, y_s, y_r,
):
    r = lax.axis_index("row")
    ga = lax.axis_index("ga")
    levels = []
    while 1 << len(levels) < rows_n:
        levels.append(1 << len(levels))
    order_a = levels
    order_b = levels[:1] + levels[2:3] + levels[1:2] + levels[3:]
    order_c = levels

    def other(index, j):
        for b in levels:
            if j & b:
                index = index + b - 2 * b * ((r // b) % 2)
        return index

    def k_of(j):
        return other(r, j)

    loads = [
        pltpu.make_async_copy(src, dst, load_sem.at[i])
        for i, (src, dst) in enumerate(
            (
                (pd_hbm, pd),
                (val_hbm, val),
                (w_hbm.at[:, cut:, :], w_b),
                (w_hbm.at[:, :cut, :], w_a),
                (cond_hbm, cond),
            )
        )
    ]
    for load in loads:
        load.start()

    barrier = pltpu.get_barrier_semaphore()
    for b in levels:
        pl.semaphore_signal(
            barrier, inc=1, device_id={"row": k_of(b), "ga": ga}, device_id_type=MESH
        )
    for d in range(1, ga_n):
        pl.semaphore_signal(
            barrier, inc=1, device_id={"row": r, "ga": (ga + d) % ga_n}, device_id_type=MESH
        )
    pl.semaphore_wait(barrier, len(levels) + ga_n - 1)

    started = []

    def send(src, dst, ssem, rsem, b):
        copy = pltpu.make_async_remote_copy(
            src_ref=src, dst_ref=dst, send_sem=ssem, recv_sem=rsem,
            device_id={"row": k_of(b), "ga": ga}, device_id_type=MESH,
        )
        copy.start()
        started.append(copy)
        return copy

    copies = {}

    def gather_terms(acc, name, recv, order, j):
        for b in order:
            if j & b:
                return acc, b
            copies[name, j | b].wait_recv()
            acc = acc + recv[j | b].astype(acc.dtype)
        return acc, 0

    column = column_ref[0]
    loads[0].wait()
    is_root = column == r

    def finish_c(j):
        own = pd[k_of(j)]
        own = jnp.where(is_root, own, jnp.zeros_like(own))
        acc, b = gather_terms(own, "c", recv_c, order_c, j)
        if j == 0:
            col[r] = acc
            return
        send_c[j] = acc
        copies["c", j] = send(send_c.at[j], recv_c.at[j], sc_s.at[j], sc_r.at[j], b)

    streams = {
        "a": (order_a, w_a, part_a, send_a, recv_a, sa_s, sa_r, t_a),
        "b": (order_b, w_b, part_b, send_b, recv_b, sb_s, sb_r, t_b),
    }

    def finish(name, j, acc=None):
        order, _, part, outgoing, recv, ssem, rsem, result = streams[name]
        if acc is None:
            acc, b = gather_terms(part[j // 2], name, recv, order[1:], j)
        else:
            b = first_of(order, j)
        if j == 0:
            result[...] = acc.astype(BF)
            return
        outgoing[j] = acc.astype(BF)
        copies[name, j] = send(outgoing.at[j], recv.at[j], ssem.at[j], rsem.at[j], b)

    def first_of(order, j):
        return [b for b in order if j & b][0]

    by_depth = sorted(range(rows_n), key=lambda j: (-bin(j).count("1"), -j))

    def first_bit(order, j):
        for at, b in enumerate(order):
            if j & b:
                return at
        return len(order)

    def level(order, at, even):
        return [j for j in by_depth if (not even or j % 2 == 0) and first_bit(order, j) == at]

    for at in (0, 1):
        for j in level(order_c, at, False):
            finish_c(j)

    evens = [j for j in by_depth if j % 2 == 0]

    def partial(name, j):
        k = k_of(j)
        weights = streams[name][1]
        return lax.dot_general(val[k], weights[q_ref[k]], NT, preferred_element_type=F32)

    def even_step(name, j):
        order, _, part, _, recv = streams[name][:5]
        value = partial(name, j)
        copies[name, j + 1].wait_recv()
        value = value + recv[j + 1].astype(F32)
        if j and first_of(order, j) == order[1]:
            finish(name, j, value)
        else:
            part[j // 2] = value

    skew = 2
    loads[1].wait()
    for name, load in (("b", 2), ("a", 3)):
        loads[load].wait()
        for step in range(len(evens) + skew):
            if step < len(evens):
                finish(name, evens[step] + 1, partial(name, evens[step] + 1))
            if step >= skew:
                even_step(name, evens[step - skew])

    held = [0]
    arriving = []

    def spread(b):
        for i, copy in arriving:
            copy.wait_recv()
            held.append(i)
        arriving.clear()
        for i in held if b else []:
            k = k_of(i)
            arriving.append(
                (i | b, send(col.at[k], col.at[k], g_s.at[i | b], g_r.at[i | b], b))
            )

    for at in range(2, len(levels)):
        for j in level(order_c, at, False):
            finish_c(j)
        for one, two in zip(level(order_a, at, True), level(order_b, at, True)):
            finish("a", one)
            if at == len(levels) - 1:
                finish_c(0)
                spread(levels[-1])
            finish("b", two)
    for b in reversed(levels[:-1]):
        spread(b)
    spread(0)

    slots = NV * NC
    h = pd.shape[-1]
    weighted = (pd[...].reshape(slots, h).astype(F32) * coul_ref[...].astype(F32).reshape(1, h)).astype(BF)
    exch = 2.0 * lax.dot_general(
        weighted, col[...].reshape(slots, h), NT, preferred_element_type=F32
    )
    my_pairs = pairs_ref[pl.ds(r, 1), :]
    col_pairs = pairs_ref[pl.ds(column, 1), :]
    place = lax.broadcasted_iota(jnp.int32, (slots, slots), 0)

    def pick(wanted):
        return jnp.where(place == wanted, 1.0, 0.0).astype(F32)

    rows_of = pick(my_pairs).T.astype(BF)
    rows_of_direct = pick((my_pairs % NC) * NV + my_pairs // NC).T.astype(BF)
    cols_of = pick(col_pairs).astype(BF)

    def chosen(left, value):
        high, low = split(value)
        return jnp.dot(left, high, preferred_element_type=F32) + jnp.dot(
            left, low, preferred_element_type=F32
        )

    total = chosen(rows_of, exch)

    vv = NV * NV
    row_id = lax.broadcasted_iota(jnp.int32, (vv, vv), 0)
    col_id = lax.broadcasted_iota(jnp.int32, (vv, vv), 1)
    swap = jnp.where(col_id == (row_id % NV) * NV + row_id // NV, 1.0, 0.0).astype(BF)

    def direct_of(valence, conduction):
        swapped = jnp.dot(swap, valence, preferred_element_type=F32).astype(BF)
        return lax.dot_general(swapped, conduction, NT, preferred_element_type=F32)

    loads[4].wait()
    finish("b", 0)
    direct = direct_of(t_b[...], cond[:, cut:])
    finish("a", 0)
    direct = direct + direct_of(t_a[...], cond[:, :cut])
    arranged = jnp.concatenate(
        [
            jnp.concatenate(
                [
                    direct[vp * NV:(vp + 1) * NV, c * NC:(c + 1) * NC]
                    for vp in range(NV)
                ],
                axis=1,
            )
            for c in range(NC)
        ],
        axis=0,
    )
    total = total - chosen(rows_of_direct, arranged)
    high, low = split(total)
    total = jnp.dot(high, cols_of, preferred_element_type=F32) + jnp.dot(
        low, cols_of, preferred_element_type=F32
    )
    width = slots // ga_n
    for g in range(ga_n):
        piece = total[:, g * width:(g + 1) * width]
        own[g] = piece
        kp[g] = piece.astype(BF)
    finals = []
    for d in range(1, ga_n):
        to = (ga + d) % ga_n
        copy = pltpu.make_async_remote_copy(
            src_ref=kp.at[to], dst_ref=kr.at[d - 1], send_sem=y_s.at[d - 1], recv_sem=y_r.at[d - 1],
            device_id={"row": r, "ga": to}, device_id_type=MESH,
        )
        copy.start()
        finals.append(copy)
    acc = own[ga]
    for d, copy in enumerate(finals):
        copy.wait_recv()
        acc = acc + kr[d].astype(F32)
    srow = lax.broadcasted_iota(jnp.int32, (slots, width), 0)
    tcol = lax.broadcasted_iota(jnp.int32, (slots, width), 1) + ga * width
    active = (srow < counts_ref[r]) & (tcol < counts_ref[column])
    out_ref[...] = jnp.where(active, acc, 0.0).astype(BF)
    for copy in started + finals:
        copy.wait_send()


def solution(mesh):
    rows_n, ga_n = mesh.shape["row"], mesh.shape["ga"]

    def per_device(
        pair_dens, cond_dens, val_dens, screened, coulomb, pair_list, counts, q_index, column_k
    ):
        slots, h = pair_dens.shape[1:]
        vv = val_dens.shape[1]
        cut = max(128, (h * 5 // 8) // 128 * 128)
        chunk = slots // rows_n
        half = rows_n // 2
        vmem = pl.BlockSpec(memory_space=pltpu.VMEM)
        smem = pl.BlockSpec(memory_space=pltpu.SMEM)
        hbm = pl.BlockSpec(memory_space=pl.ANY)
        dma = pltpu.SemaphoreType.DMA
        return pl.pallas_call(
            functools.partial(kernel, rows_n, ga_n, cut),
            out_shape=jax.ShapeDtypeStruct((slots, slots // ga_n), BF),
            in_specs=[hbm, hbm, hbm, hbm, vmem, vmem, smem, smem, smem],
            out_specs=vmem,
            scratch_shapes=[
                pltpu.VMEM((rows_n, chunk, h), BF),
                pltpu.VMEM(cond_dens.shape[1:], BF),
                pltpu.VMEM(val_dens.shape, BF),
                pltpu.VMEM((screened.shape[0], cut, screened.shape[2]), BF),
                pltpu.VMEM((screened.shape[0], h - cut, screened.shape[2]), BF),
                pltpu.VMEM((half, vv, cut), F32),
                pltpu.VMEM((half, vv, h - cut), F32),
                pltpu.VMEM((rows_n, vv, cut), BF),
                pltpu.VMEM((rows_n, vv, h - cut), BF),
                pltpu.VMEM((rows_n, vv, cut), BF),
                pltpu.VMEM((rows_n, vv, h - cut), BF),
                pltpu.VMEM((rows_n, chunk, h), BF),
                pltpu.VMEM((rows_n, chunk, h), BF),
                pltpu.VMEM((rows_n, chunk, h), BF),
                pltpu.VMEM((vv, cut), BF),
                pltpu.VMEM((vv, h - cut), BF),
                pltpu.VMEM((ga_n, slots, slots // ga_n), F32),
                pltpu.VMEM((ga_n, slots, slots // ga_n), BF),
                pltpu.VMEM((max(1, ga_n - 1), slots, slots // ga_n), BF),
                dma((5,)),
                dma((rows_n,)), dma((rows_n,)),
                dma((rows_n,)), dma((rows_n,)),
                dma((rows_n,)), dma((rows_n,)),
                dma((rows_n,)), dma((rows_n,)),
                dma((max(1, ga_n - 1),)), dma((max(1, ga_n - 1),)),
            ],
            compiler_params=pltpu.CompilerParams(
                collective_id=0, has_side_effects=True, vmem_limit_bytes=60 * 1024 * 1024
            ),
        )(
            pair_dens.reshape(rows_n, chunk, h),
            cond_dens.reshape(cond_dens.shape[1:]),
            val_dens,
            screened,
            coulomb,
            pair_list,
            counts,
            q_index,
            column_k,
        )

    placed = (
        P("row", None, "ga"),
        P("row", None, "ga"),
        P(None, None, "row"),
        P(None, "ga", "row"),
        P("ga"),
        P(),
        P(),
        P(),
        P(),
    )
    return jax.shard_map(
        per_device, mesh=mesh, in_specs=placed, out_specs=P("row", "ga"), check_vma=False
    )
```
